32 devices in a mesh: row: 4 (over y, x), col: 8 (over z, core).
Axes of the slice: x: 2, y: 2, z: 4, core: 2. Of those that a mesh axis runs over, the one named last changes fastest.
Arguments:
- matrix: float32 [32, 4, 128, 16, 8, 128], P(None, 'row', None, None, 'col'), as said below
Outputs:
- updated: float32 [32, 4, 128, 16, 8, 128], P(None, 'row', None, None, 'col')
- images: float32 [8, 32, 4, 128], P(None, None, 'row')
Inputs may be any that keep to these rules, and one draw needn't show every extreme that they name: The matrix is symmetric: entry (r, c) equals entry (c, r).
All inputs are finite; a program needn't handle non-finite values.
Results may differ from the reference program's by a relative error of at most 0.00016.
Values sent between devices are 32-bit elements; how exact they have to be, the bound alone decides.
A program may use at most 192 MiB of HBM per device.

```python
import math
import jax
import jax.numpy as jnp
from jax import lax

N = 16384
NB = 128
K = 8
LR = 32
LC = 16
N_ROW = 4
N_COL = 8


def draw_matrix(key, part):
    first_key = jax.random.fold_in(key, 11)
    row_ids = jnp.arange(N, dtype=jnp.int32)
    block_pos = (row_ids // NB % N_ROW).astype(jnp.float32) / (N_ROW - 1)
    base_scale = jnp.exp((block_pos - 0.5) * math.log(3.0))
    entries = jax.random.truncated_normal(first_key, -6.0, 6.0, (N, N), jnp.float32)
    row_scale = base_scale
    symmetric = (entries + entries.T) * 0.70710678
    scaled = row_scale[:, None] * symmetric * row_scale[None, :]
    return scaled.reshape(LR, N_ROW, NB, LC, N_COL, NB)


def setup_inputs(seed: int = 0) -> dict:
    key_of = jax.random.split(jax.random.key(seed), 2)
    return {
        "matrix": draw_matrix(jax.random.fold_in(key_of[1], 71), 0),
    }


epsilon = 1e-06
highest = lax.Precision.HIGHEST

def product(left_side, right_side):
    return jnp.dot(left_side, right_side, precision=highest)

def reference(matrix):
    square = matrix.reshape(N, N)
    row_ids = jnp.arange(N, dtype=jnp.int32)
    reflectors = jnp.zeros((N, K), jnp.float32)
    images_mat = jnp.zeros((N, K), jnp.float32)
    for position in range(K):
        column = square[:, position] - product(reflectors, images_mat[position]) - product(images_mat, reflectors[position])
        below_diag = jnp.where(row_ids > position, column, jnp.zeros_like(column))
        col_norm = jnp.sqrt(jnp.sum(below_diag * below_diag))
        first_entry = column[position + 1]
        vector = below_diag + jnp.where(row_ids == position + 1, col_norm, jnp.zeros_like(column))
        reflector = vector / jnp.sqrt(2.0 * col_norm * (col_norm + first_entry) + epsilon)
        image_vec = product(square, reflector) - product(reflectors, product(images_mat.T, reflector)) - product(images_mat, product(reflectors.T, reflector))
        gamma_val = product(reflector, image_vec)
        update = 2.0 * image_vec - 2.0 * gamma_val * reflector
        reflectors = reflectors.at[:, position].set(reflector)
        images_mat = images_mat.at[:, position].set(update)
    left_side = jnp.concatenate([reflectors, images_mat], axis=1)
    right_side = jnp.concatenate([images_mat, reflectors], axis=1)
    updated = square - product(left_side, right_side.T)
    return (updated.reshape(matrix.shape), images_mat.T.reshape(K, LR, N_ROW, NB))
```

```python
import functools

import jax
import jax.numpy as jnp
from jax import lax
from jax.experimental import pallas as pl
from jax.experimental.pallas import tpu as pltpu
from jax.sharding import PartitionSpec as P

K = 8
epsilon = 1e-06
MESH = pl.DeviceIdType.MESH
WIDE = 16384.0


def total(values):
    rows = jnp.sum(values, axis=0)
    lanes = jnp.sum(rows, axis=0, keepdims=True)
    return jnp.sum(lanes, axis=1, keepdims=True)


def spread(value):
    return value.reshape(1, 1, 1)


def peak(values):
    rows = jnp.max(jnp.abs(values), axis=0)
    lanes = jnp.max(rows, axis=0, keepdims=True)
    return jnp.max(lanes, axis=1, keepdims=True)


def panel_kernel(
    row_count,
    col_count,
    row_blocks,
    col_blocks,
    block,
    span,
    a_hbm,
    tile,
    left_ref,
    right_ref,
    v_ref,
    w_ref,
    pan,
    ub,
    part,
    got,
    full,
    carry_ref,
    fix_ref,
    base_ref,
    rate_ref,
    load_sem,
    own_sem,
    down_send,
    down_recv,
    pan_send,
    pan_recv,
    part_send,
    part_recv,
    full_send,
    full_recv,
):
    p = lax.axis_index("row")
    q = lax.axis_index("col")
    ratio = col_count // row_count
    owner = lax.rem(q, row_count)
    rank = q // row_count
    mine = owner * ratio + rank
    local = owner == p

    def load(i, c):
        blocks = pl.ds(i * span, span)
        return pltpu.make_async_copy(
            a_hbm.at[blocks, :, c], tile.at[c, blocks], load_sem.at[i]
        )

    own = pltpu.make_async_copy(a_hbm.at[0, pl.ds(0, K + 1)], pan.at[mine], own_sem)

    @pl.when(p == 0)
    def _():
        own.start()

    barrier = pltpu.get_barrier_semaphore()

    def greet(row, col):
        pl.semaphore_signal(barrier, inc=1, device_id=(row, col), device_id_type=MESH)

    for d in range(1, row_count):
        greet(lax.rem(p + d, row_count), q)
    for d in range(1, col_count):
        greet(p, lax.rem(q + d, col_count))
    for d in range(1, col_count):
        greet(owner, lax.rem(q + d, col_count))
    for r in range(row_count):
        for k in range(ratio):
            source = p + k * row_count

            @pl.when(jnp.logical_or(p != r, q != source))
            def _():
                greet(r, source)

    @pl.when(jnp.logical_not(local))
    def _():
        greet(owner, q)

    def start_load(i, carry):
        for c in range(col_blocks):
            load(i, c).start()
        return carry

    lax.fori_loop(0, row_blocks // span, start_load, 0)
    v_ref[...] = jnp.zeros_like(v_ref)
    w_ref[...] = jnp.zeros_like(w_ref)
    carry_ref[...] = jnp.zeros_like(carry_ref)
    rate_ref[...] = jnp.ones_like(rate_ref)
    own_part = jnp.where(local, 1, 0)
    pl.semaphore_wait(barrier, row_count + col_count - 2 + 2 * (col_count - own_part))

    pieces = (pl.ds(0, 1), pl.ds(1, K))

    def down(d, i):
        return pltpu.make_async_remote_copy(
            src_ref=pan.at[mine, pieces[i]],
            dst_ref=pan.at[mine, pieces[i]],
            send_sem=down_send.at[d, i],
            recv_sem=down_recv.at[i],
            device_id=(d, q),
            device_id_type=MESH,
        )

    def across(d, i, slot):
        return pltpu.make_async_remote_copy(
            src_ref=pan.at[slot, pieces[i]],
            dst_ref=pan.at[slot, pieces[i]],
            send_sem=pan_send.at[d, i],
            recv_sem=pan_recv.at[slot, i],
            device_id=(p, lax.rem(q + d, col_count)),
            device_id_type=MESH,
        )

    def across_recv(i):
        for d in range(1, col_count):
            other = lax.rem(q + d, col_count)
            across(d, i, lax.rem(other, row_count) * ratio + other // row_count).wait_recv()

    @pl.when(p == 0)
    def _():
        own.wait()
        for i in range(2):
            for d in range(1, row_count):
                down(d, i).start()

    for i in range(2):

        @pl.when(p != 0)
        def _():
            down(0, i).wait_recv()

        for d in range(1, col_count):
            across(d, i, mine).start()

    shape = (col_count, col_blocks, block)
    slot_id = lax.broadcasted_iota(jnp.int32, shape, 0)
    block_id = (
        lax.broadcasted_iota(jnp.int32, shape, 1) * col_count
        + lax.rem(slot_id, ratio) * row_count
        + slot_id // ratio
    )
    ids = block_id * block + lax.broadcasted_iota(jnp.int32, shape, 2)
    lane = lax.broadcasted_iota(jnp.int32, (1, block), 1)
    piece_ids = [
        (lax.broadcasted_iota(jnp.int32, shape[1:], 0) * col_count + k * row_count + p) * block
        + lax.broadcasted_iota(jnp.int32, shape[1:], 1)
        for k in range(ratio)
    ]

    def entry(row, i):
        return jnp.sum(jnp.where(lane == i, row, 0.0), axis=1, keepdims=True)

    def lay(values, scale):
        for k in range(ratio):
            turned = values[k].T
            if scale is not None:
                turned = turned * scale
            for b in range(col_blocks):
                a = b * ratio + k
                ub[a * block : (a + 1) * block, :] = jnp.broadcast_to(
                    turned[:, b : b + 1], (block, block)
                )

    def reflect(column, j):
        below = jnp.where(ids > j, column, 0.0)
        norm = jnp.sqrt(total(below * below))
        first = entry(column[0, 0:1, :], j + 1)
        denom = jnp.sqrt(2.0 * norm * (norm + first) + epsilon)
        u = (below + jnp.where(ids == j + 1, spread(norm), 0.0)) / spread(denom)
        v_ref[j] = u
        return norm, denom

    across_recv(0)
    reflect(pan[:, 0], 0)
    lay([v_ref[0, p * ratio + k] for k in range(ratio)], None)

    def send_part(j, d):
        return pltpu.make_async_remote_copy(
            src_ref=part.at[j],
            dst_ref=got.at[j, p * ratio + rank],
            send_sem=part_send.at[j, d],
            recv_sem=part_recv.at[j, p * ratio + rank],
            device_id=(owner, lax.rem(q + d, col_count)),
            device_id_type=MESH,
        )

    def recv_part(j, r, k):
        slot = r * ratio + k
        return pltpu.make_async_remote_copy(
            src_ref=part.at[j],
            dst_ref=got.at[j, slot],
            send_sem=part_send.at[j, 0],
            recv_sem=part_recv.at[j, slot],
            device_id=(r, p + k * row_count),
            device_id_type=MESH,
        )

    def full_copy(j, d, slot):
        return pltpu.make_async_remote_copy(
            src_ref=full.at[j, pl.ds(slot * ratio, ratio)],
            dst_ref=full.at[j, pl.ds(slot * ratio, ratio)],
            send_sem=full_send.at[j, d],
            recv_sem=full_recv.at[j, slot],
            device_id=(lax.rem(p + d, row_count), q),
            device_id_type=MESH,
        )

    def full_wait(j):
        for d in range(1, row_count):
            full_copy(j, d, lax.rem(p + d, row_count)).wait_recv()

    def image_of(i):
        u = v_ref[i]
        product = full[i] + carry_ref[...]
        image = product - fix_ref[...]
        gamma = total(u * image)
        update = 2.0 * image - spread(2.0 * gamma) * u
        w_ref[i] = update
        return u, product, gamma, update

    def step(j, beta):
        @pl.when(j == 0)
        def _():
            def arrive(i, carry):
                pltpu.make_async_copy(
                    tile.at[:, pl.ds(i * span, span)],
                    tile.at[:, pl.ds(i * span, span)],
                    load_sem.at[i],
                ).wait()
                return carry

            lax.fori_loop(0, row_blocks // span, arrive, 0)

        def gather(a, acc):
            out = list(acc)
            first_row = pl.multiple_of(a * block, block)
            for r in range(0, block, 8):
                scale = ub[pl.ds(first_row + r, 8), :]
                for c in range(col_blocks):
                    out[c] = out[c] + tile[c, a, r : r + 8, :] * scale
            return tuple(out)

        acc = lax.fori_loop(
            0,
            row_blocks,
            gather,
            tuple(jnp.zeros((8, block), jnp.float32) for _ in range(col_blocks)),
        )
        for c in range(col_blocks):
            part[j, c : c + 1, :] = jnp.sum(acc[c], axis=0, keepdims=True)

        for d in range(1, col_count):
            send_part(j, d).start()

        @pl.when(jnp.logical_not(local))
        def _():
            send_part(j, 0).start()

        @pl.when(local)
        def _():
            got[j, mine] = part[j]

        @pl.when(j == 0)
        def _():
            across_recv(1)

        @pl.when(j > 0)
        def _():
            i = j - 1
            full_wait(i)
            trial = base_ref[...] - spread(beta) * full[i]
            inner = jnp.where(ids > j, trial, 0.0)
            u, product, gamma, update = image_of(i)
            sigma = beta * gamma - entry(update[0, 0:1, :], j)
            norm, denom = reflect(trial + spread(sigma) * u, j)
            carry_ref[...] = spread(sigma / denom) * (
                product - spread(0.5 * beta) * pan[:, j]
            ) + spread(norm / denom) * pan[:, j + 1]
            for r in range(row_count):
                top = peak(inner[r * ratio : (r + 1) * ratio])
                top = jnp.where(top > 0.0, top, 1.0)
                rate_ref[r : r + 1, :] = jnp.broadcast_to(top * (WIDE / denom), (1, block))

        u = v_ref[j]
        beta = 2.0 * entry(u[0, 0:1, :], j + 1)
        fix = jnp.zeros(shape, jnp.float32)
        column = pan[:, j + 1]
        for t in range(K):
            v_t, w_t = v_ref[t], w_ref[t]
            fix = fix + v_t * spread(total(w_t * u)) + w_t * spread(total(v_t * u))
            v_j = entry(v_ref[t, 0, 0:1, :], j + 1)
            w_j = entry(w_ref[t, 0, 0:1, :], j + 1)
            column = column - v_t * spread(w_j) - w_t * spread(v_j)
        fix_ref[...] = fix
        base_ref[...] = column + spread(beta) * (fix - carry_ref[...])

        for r in range(row_count):
            for k in range(ratio):

                @pl.when(jnp.logical_or(p != r, q != p + k * row_count))
                def _():
                    recv_part(j, r, k).wait_recv()

        news = []
        for k in range(ratio):
            new = got[j, k] * rate_ref[0:1, :]
            for r in range(1, row_count):
                new = new + got[j, r * ratio + k] * rate_ref[r : r + 1, :]
            full[j, p * ratio + k] = new
            news.append(new)
        for d in range(1, row_count):
            full_copy(j, d, p).start()

        @pl.when(j < K - 1)
        def _():
            values = [
                jnp.where(
                    piece_ids[k] > j + 1, base_ref[p * ratio + k] - beta * news[k], 0.0
                )
                for k in range(ratio)
            ]
            top = peak(jnp.stack(values))
            top = jnp.where(top > 0.0, top, 1.0)
            lay(values, (1.0 / WIDE) / top)

        for d in range(1, col_count):
            send_part(j, d).wait_send()

        @pl.when(jnp.logical_not(local))
        def _():
            send_part(j, 0).wait_send()

        return beta

    lax.fori_loop(0, K, step, jnp.zeros((1, 1), jnp.float32))
    full_wait(K - 1)
    image_of(K - 1)
    for t in range(K):
        for k in range(ratio):
            left_ref[t, pl.ds(k, col_blocks, stride=ratio), :] = v_ref[t, p * ratio + k]
            left_ref[K + t, pl.ds(k, col_blocks, stride=ratio), :] = w_ref[t, p * ratio + k]
        right_ref[t] = w_ref[t, mine]
        right_ref[K + t] = v_ref[t, mine]

    def drain(j, carry):
        for d in range(1, row_count):
            full_copy(j, d, p).wait_send()
        return carry

    lax.fori_loop(0, K, drain, 0)
    for i in range(2):
        for d in range(1, col_count):
            across(d, i, mine).wait_send()

    @pl.when(p == 0)
    def _():
        for i in range(2):
            for d in range(1, row_count):
                down(d, i).wait_send()


def split(values):
    high = values.astype(jnp.bfloat16)
    low = (values - high.astype(jnp.float32)).astype(jnp.bfloat16)
    return high, low


def update_kernel(row_blocks, col_blocks, block, span, tile, left_ref, right_ref, out_hbm, image_ref, buf, sem):
    image_ref[...] = left_ref[K:]
    right_high, right_low = split(
        jnp.concatenate([right_ref[:, c, :] for c in range(col_blocks)], axis=1)
    )
    right = jnp.concatenate([right_high, right_low, right_high], axis=0)
    rows = span * block

    def out(i, c):
        slot = lax.rem(i, 2)
        return pltpu.make_async_copy(
            buf.at[slot, c], out_hbm.at[pl.ds(i * span, span), :, c], sem.at[slot, c]
        )

    def chunk(i, carry):
        slot = lax.rem(i, 2)
        left_high, left_low = split(
            jnp.concatenate([left_ref[:, i * span + s, :] for s in range(span)], axis=1)
        )
        left = jnp.concatenate([left_high, left_high, left_low], axis=0)

        for c in range(0, col_blocks, 2):

            @pl.when(i >= 2)
            def _():
                out(i - 2, c).wait()
                out(i - 2, c + 1).wait()

            change = lax.dot_general(
                left,
                right[:, c * block : (c + 2) * block],
                (((0,), (0,)), ((), ())),
                preferred_element_type=jnp.float32,
            )
            for e in range(2):
                buf[slot, c + e] = tile[c + e, pl.ds(i * span, span)] - change[
                    :, e * block : (e + 1) * block
                ].reshape(span, block, block)
                out(i, c + e).start()
        return carry

    steps = row_blocks // span
    lax.fori_loop(0, steps, chunk, 0)
    for i in range(max(steps - 2, 0), steps):
        for c in range(col_blocks):
            out(i, c).wait()


def body(row_count, col_count, matrix):
    row_blocks, _, block, col_blocks, _, _ = matrix.shape
    grid = matrix.reshape(row_blocks, block, col_blocks, block)
    vec = (col_count, col_blocks, block)
    dma = pltpu.SemaphoreType.DMA
    span = max(row_blocks // 8, 1)
    tile, left, right = pl.pallas_call(
        functools.partial(
            panel_kernel, row_count, col_count, row_blocks, col_blocks, block, span
        ),
        out_shape=[
            pltpu.VMEM((col_blocks, row_blocks, block, block), jnp.float32),
            pltpu.VMEM((2 * K, row_blocks, block), jnp.float32),
            pltpu.VMEM((2 * K, col_blocks, block), jnp.float32),
        ],
        in_specs=[pl.BlockSpec(memory_space=pl.ANY)],
        out_specs=[pl.BlockSpec(memory_space=pltpu.VMEM)] * 3,
        scratch_shapes=[
            pltpu.VMEM((K,) + vec, jnp.float32),
            pltpu.VMEM((K,) + vec, jnp.float32),
            pltpu.VMEM((col_count, K + 1, col_blocks, block), jnp.float32),
            pltpu.VMEM((row_blocks * block, block), jnp.float32),
            pltpu.VMEM((K, col_blocks, block), jnp.float32),
            pltpu.VMEM((K,) + vec, jnp.float32),
            pltpu.VMEM((K,) + vec, jnp.float32),
            pltpu.VMEM(vec, jnp.float32),
            pltpu.VMEM(vec, jnp.float32),
            pltpu.VMEM(vec, jnp.float32),
            pltpu.VMEM((max(row_count, 8), block), jnp.float32),
            dma((row_blocks // span,)),
            dma,
            dma((row_count, 2)),
            dma((2,)),
            dma((col_count, 2)),
            dma((col_count, 2)),
            dma((K, col_count)),
            dma((K, col_count)),
            dma((K, row_count)),
            dma((K, row_count)),
        ],
        compiler_params=pltpu.CompilerParams(
            collective_id=0, has_side_effects=True, vmem_limit_bytes=14 * 2**20
        ),
    )(grid)

    updated, images = pl.pallas_call(
        functools.partial(update_kernel, row_blocks, col_blocks, block, span),
        out_shape=[
            jax.ShapeDtypeStruct(grid.shape, jnp.float32),
            jax.ShapeDtypeStruct((K, row_blocks, block), jnp.float32),
        ],
        in_specs=[pl.BlockSpec(memory_space=pltpu.VMEM)] * 3,
        out_specs=[
            pl.BlockSpec(memory_space=pl.ANY),
            pl.BlockSpec(memory_space=pltpu.VMEM),
        ],
        scratch_shapes=[
            pltpu.VMEM((2, col_blocks, span, block, block), jnp.float32),
            dma((2, col_blocks)),
        ],
        compiler_params=pltpu.CompilerParams(vmem_limit_bytes=14 * 2**20),
    )(tile, left, right)
    return (updated.reshape(matrix.shape), images.reshape(K, row_blocks, 1, block))


def solution(mesh):
    placed = (P(None, "row", None, None, "col", None),)
    return jax.shard_map(
        functools.partial(body, mesh.shape["row"], mesh.shape["col"]),
        mesh=mesh,
        in_specs=placed,
        out_specs=(P(None, "row", None, None, "col", None), P(None, None, "row", None)),
        check_vma=False,
    )
```

```python
import functools

import jax
import jax.numpy as jnp
from jax import lax
from jax.experimental import pallas as pl
from jax.experimental.pallas import tpu as pltpu
from jax.sharding import PartitionSpec as P

K = 8
epsilon = 1e-06
MESH = pl.DeviceIdType.MESH
WIDE = 16384.0


def total(values):
    rows = jnp.sum(values, axis=0)
    lanes = jnp.sum(rows, axis=0, keepdims=True)
    return jnp.sum(lanes, axis=1, keepdims=True)


def spread(value):
    return value.reshape(1, 1, 1)


def peak(values):
    rows = jnp.max(jnp.abs(values), axis=0)
    lanes = jnp.max(rows, axis=0, keepdims=True)
    return jnp.max(lanes, axis=1, keepdims=True)


def panel_kernel(
    row_count,
    col_count,
    row_blocks,
    col_blocks,
    block,
    batch,
    a_hbm,
    tile,
    left_ref,
    right_ref,
    v_ref,
    w_ref,
    pan,
    wide_ref,
    part,
    got,
    full,
    carry_ref,
    fix_ref,
    base_ref,
    rate_ref,
    load_sem,
    own_sem,
    down_send,
    down_recv,
    pan_send,
    pan_recv,
    part_send,
    part_recv,
    full_send,
    full_recv,
):
    p = lax.axis_index("row")
    q = lax.axis_index("col")
    ratio = col_count // row_count
    owner = lax.rem(q, row_count)
    rank = q // row_count
    mine = owner * ratio + rank
    local = owner == p
    span = batch * ratio
    groups = col_blocks // batch

    def load(i, c):
        blocks = pl.ds(i * span, span)
        return pltpu.make_async_copy(
            a_hbm.at[blocks, :, c], tile.at[c, blocks], load_sem.at[i]
        )

    own = pltpu.make_async_copy(a_hbm.at[0, pl.ds(0, K + 1)], pan.at[mine], own_sem)

    @pl.when(p == 0)
    def _():
        own.start()

    barrier = pltpu.get_barrier_semaphore()

    def greet(row, col):
        pl.semaphore_signal(barrier, inc=1, device_id=(row, col), device_id_type=MESH)

    for d in range(1, row_count):
        greet(lax.rem(p + d, row_count), q)
    for d in range(1, col_count):
        greet(p, lax.rem(q + d, col_count))
    for d in range(1, col_count):
        greet(owner, lax.rem(q + d, col_count))
    for r in range(row_count):
        for k in range(ratio):
            source = p + k * row_count

            @pl.when(jnp.logical_or(p != r, q != source))
            def _():
                greet(r, source)

    @pl.when(jnp.logical_not(local))
    def _():
        greet(owner, q)

    def start_load(i, carry):
        for c in range(col_blocks):
            load(i, c).start()
        return carry

    lax.fori_loop(0, groups, start_load, 0)
    v_ref[...] = jnp.zeros_like(v_ref)
    w_ref[...] = jnp.zeros_like(w_ref)
    carry_ref[...] = jnp.zeros_like(carry_ref)
    rate_ref[...] = jnp.ones_like(rate_ref)
    own_part = jnp.where(local, 1, 0)
    pl.semaphore_wait(barrier, row_count + col_count - 2 + 2 * (col_count - own_part))

    pieces = (pl.ds(0, 1), pl.ds(1, K))

    def down(d, i):
        return pltpu.make_async_remote_copy(
            src_ref=pan.at[mine, pieces[i]],
            dst_ref=pan.at[mine, pieces[i]],
            send_sem=down_send.at[d, i],
            recv_sem=down_recv.at[i],
            device_id=(d, q),
            device_id_type=MESH,
        )

    def across(d, i, slot):
        return pltpu.make_async_remote_copy(
            src_ref=pan.at[slot, pieces[i]],
            dst_ref=pan.at[slot, pieces[i]],
            send_sem=pan_send.at[d, i],
            recv_sem=pan_recv.at[slot, i],
            device_id=(p, lax.rem(q + d, col_count)),
            device_id_type=MESH,
        )

    def across_recv(i):
        for d in range(1, col_count):
            other = lax.rem(q + d, col_count)
            across(d, i, lax.rem(other, row_count) * ratio + other // row_count).wait_recv()

    @pl.when(p == 0)
    def _():
        own.wait()
        for i in range(2):
            for d in range(1, row_count):
                down(d, i).start()

    for i in range(2):

        @pl.when(p != 0)
        def _():
            down(0, i).wait_recv()

        for d in range(1, col_count):
            across(d, i, mine).start()

    shape = (col_count, col_blocks, block)
    slot_id = lax.broadcasted_iota(jnp.int32, shape, 0)
    block_id = (
        lax.broadcasted_iota(jnp.int32, shape, 1) * col_count
        + lax.rem(slot_id, ratio) * row_count
        + slot_id // ratio
    )
    ids = block_id * block + lax.broadcasted_iota(jnp.int32, shape, 2)
    lane = lax.broadcasted_iota(jnp.int32, (1, block), 1)
    def entry(row, i):
        return jnp.sum(jnp.where(lane == i, row, 0.0), axis=1, keepdims=True)

    def keep(ref, t, left_row, right_row):
        for k in range(ratio):
            left_ref[left_row, pl.ds(k, col_blocks, stride=ratio), :] = ref[t, p * ratio + k]
        right_ref[right_row] = ref[t, mine]

    def reflect(column, j):
        below = jnp.where(ids > j, column, 0.0)
        norm = jnp.sqrt(total(below * below))
        first = entry(column[0, 0:1, :], j + 1)
        denom = jnp.sqrt(2.0 * norm * (norm + first) + epsilon)
        u = (below + jnp.where(ids == j + 1, spread(norm), 0.0)) / spread(denom)
        v_ref[j] = u
        keep(v_ref, j, j, K + j)
        return norm, denom

    across_recv(0)
    reflect(pan[:, 0], 0)

    def send_part(j, d):
        return pltpu.make_async_remote_copy(
            src_ref=part.at[j],
            dst_ref=got.at[j, p * ratio + rank],
            send_sem=part_send.at[j, d],
            recv_sem=part_recv.at[j, p * ratio + rank],
            device_id=(owner, lax.rem(q + d, col_count)),
            device_id_type=MESH,
        )

    def recv_part(j, r, k):
        slot = r * ratio + k
        return pltpu.make_async_remote_copy(
            src_ref=part.at[j],
            dst_ref=got.at[j, slot],
            send_sem=part_send.at[j, 0],
            recv_sem=part_recv.at[j, slot],
            device_id=(r, p + k * row_count),
            device_id_type=MESH,
        )

    def full_copy(j, d, slot):
        return pltpu.make_async_remote_copy(
            src_ref=full.at[j, pl.ds(slot * ratio, ratio)],
            dst_ref=full.at[j, pl.ds(slot * ratio, ratio)],
            send_sem=full_send.at[j, d],
            recv_sem=full_recv.at[j, slot],
            device_id=(lax.rem(p + d, row_count), q),
            device_id_type=MESH,
        )

    def full_wait(j):
        for d in range(1, row_count):
            full_copy(j, d, lax.rem(p + d, row_count)).wait_recv()

    def image_of(i):
        u = v_ref[i]
        product = full[i] + carry_ref[...]
        image = product - fix_ref[...]
        gamma = total(u * image)
        update = 2.0 * image - spread(2.0 * gamma) * u
        w_ref[i] = update
        keep(w_ref, i, K + i, i)
        return u, product, gamma, update

    def widen(k, turned):
        for b in range(col_blocks):
            wide_ref[k, b] = jnp.broadcast_to(turned[:, b : b + 1], (block, block))

    def gather(b, k, acc):
        out = list(acc)
        a = b * ratio + k
        for r in range(0, block, 8):
            scale = wide_ref[k, b, r : r + 8, :]
            for c in range(col_blocks):
                out[c] = out[c] + tile[c, a, r : r + 8, :] * scale
        return tuple(out)

    blank = tuple(jnp.zeros((8, block), jnp.float32) for _ in range(col_blocks))

    def emit(j, acc):
        for c in range(col_blocks):
            part[j, c : c + 1, :] = jnp.sum(acc[c], axis=0, keepdims=True)
        for d in range(1, col_count):
            send_part(j, d).start()

        @pl.when(jnp.logical_not(local))
        def _():
            send_part(j, 0).start()

        @pl.when(local)
        def _():
            got[j, mine] = part[j]

    for k in range(ratio):
        widen(k, v_ref[0, p * ratio + k].T)

    def opening(g, acc):
        blocks = pl.ds(g * span, span)
        pltpu.make_async_copy(tile.at[:, blocks], tile.at[:, blocks], load_sem.at[g]).wait()
        for k in range(ratio):
            acc = lax.fori_loop(
                0, batch, lambda e, acc, k=k: gather(g * batch + e, k, acc), acc, unroll=2
            )
        return acc

    emit(0, lax.fori_loop(0, groups, opening, blank))

    def gap(k):
        ahead = lax.rem(p + k * row_count - q + col_count, col_count)
        return jnp.minimum(ahead, col_count - ahead)

    first_rank, nearest = 0, gap(0)
    for k in range(1, ratio):
        first_rank = jnp.where(gap(k) < nearest, k, first_rank)
        nearest = jnp.minimum(gap(k), nearest)

    def absorb(j, k):
        for r in range(row_count):

            @pl.when(jnp.logical_or(p != r, q != p + k * row_count))
            def _():
                recv_part(j, r, k).wait_recv()

        new = got[j, k] * rate_ref[0:1, :]
        for r in range(1, row_count):
            new = new + got[j, r * ratio + k] * rate_ref[r : r + 1, :]
        full[j, p * ratio + k] = new
        return new

    def share(j):
        for d in range(1, row_count):
            full_copy(j, d, p).start()

    def positive(value):
        return jnp.where(value > 0.0, value, 1.0)

    def step(j, beta):
        @pl.when(j == 0)
        def _():
            across_recv(1)

        @pl.when(j > 0)
        def _():
            i = j - 1
            full_wait(i)
            trial = base_ref[...] - spread(beta) * full[i]
            inner = jnp.where(ids > j, trial, 0.0)
            u, product, gamma, update = image_of(i)
            sigma = beta * gamma - entry(update[0, 0:1, :], j)
            norm, denom = reflect(trial + spread(sigma) * u, j)
            carry_ref[...] = spread(sigma / denom) * (
                product - spread(0.5 * beta) * pan[:, j]
            ) + spread(norm / denom) * pan[:, j + 1]
            for r in range(row_count):
                top = positive(peak(inner[r * ratio : (r + 1) * ratio]))
                rate_ref[r : r + 1, :] = jnp.broadcast_to(top * (WIDE / denom), (1, block))

        u = v_ref[j]
        beta = 2.0 * entry(u[0, 0:1, :], j + 1)
        fix = jnp.zeros(shape, jnp.float32)
        column = pan[:, j + 1]
        for t in range(K):
            v_t, w_t = v_ref[t], w_ref[t]
            fix = fix + v_t * spread(total(w_t * u)) + w_t * spread(total(v_t * u))
            v_j = entry(v_ref[t, 0, 0:1, :], j + 1)
            w_j = entry(w_ref[t, 0, 0:1, :], j + 1)
            column = column - v_t * spread(w_j) - w_t * spread(v_j)
        fix_ref[...] = fix
        base_ref[...] = column + spread(beta) * (fix - carry_ref[...])

        @pl.when(j < K - 1)
        def _():
            acc, top = blank, None
            for h in range(ratio):
                k = lax.rem(first_rank + h, ratio)
                new = absorb(j, k)
                if h == ratio - 1:
                    share(j)
                place = (
                    lax.broadcasted_iota(jnp.int32, shape[1:], 0) * col_count + k * row_count + p
                ) * block + lax.broadcasted_iota(jnp.int32, shape[1:], 1)
                values = jnp.where(place > j + 1, base_ref[p * ratio + k] - beta * new, 0.0)
                here = peak(values[None])
                if top is None:
                    top = here
                else:
                    old = positive(top)
                    top = jnp.maximum(top, here)
                    shrink = old / positive(top)
                    acc = tuple(value * shrink for value in acc)
                widen(k, values.T * ((1.0 / WIDE) / positive(top)))
                acc = lax.fori_loop(0, col_blocks, lambda b, acc, k=k: gather(b, k, acc), acc, unroll=2)
            emit(j + 1, acc)

        @pl.when(j == K - 1)
        def _():
            for k in range(ratio):
                absorb(j, k)
            share(j)

        return beta

    lax.fori_loop(0, K, step, jnp.zeros((1, 1), jnp.float32))
    full_wait(K - 1)
    image_of(K - 1)

    def drain(j, carry):
        for d in range(1, row_count):
            full_copy(j, d, p).wait_send()
        for d in range(1, col_count):
            send_part(j, d).wait_send()

        @pl.when(jnp.logical_not(local))
        def _():
            send_part(j, 0).wait_send()

        return carry

    lax.fori_loop(0, K, drain, 0)
    for i in range(2):
        for d in range(1, col_count):
            across(d, i, mine).wait_send()

    @pl.when(p == 0)
    def _():
        for i in range(2):
            for d in range(1, row_count):
                down(d, i).wait_send()


def split(values):
    high = values.astype(jnp.bfloat16)
    low = (values - high.astype(jnp.float32)).astype(jnp.bfloat16)
    return high, low


def update_kernel(
    row_blocks, col_blocks, block, span, tile, left_ref, right_ref, out_hbm, image_ref, buf, thin, sem
):
    image_ref[...] = left_ref[K:]
    for c in range(col_blocks):
        high, low = split(right_ref[:, c, :])
        thin[:, c * block : (c + 1) * block] = jnp.concatenate([high, low, high], axis=0)

    def out(i, c):
        slot = lax.rem(i, 2)
        return pltpu.make_async_copy(
            buf.at[slot, c], out_hbm.at[pl.ds(i * span, span), :, c], sem.at[slot, c]
        )

    def chunk(i, carry):
        slot = lax.rem(i, 2)

        @pl.when(i >= 2)
        def _():
            for c in range(col_blocks):
                out(i - 2, c).wait()

        for s in range(span):
            high, low = split(left_ref[:, i * span + s, :])
            left = jnp.concatenate([high, high, low], axis=0)
            for c in range(0, col_blocks, 2):
                change = lax.dot_general(
                    left,
                    thin[:, c * block : (c + 2) * block],
                    (((0,), (0,)), ((), ())),
                    preferred_element_type=jnp.float32,
                )
                for e in range(2):
                    buf[slot, c + e, s] = (
                        tile[c + e, i * span + s] - change[:, e * block : (e + 1) * block]
                    )
        for c in range(col_blocks):
            out(i, c).start()
        return carry

    steps = row_blocks // span
    lax.fori_loop(0, steps, chunk, 0)
    for i in range(max(steps - 2, 0), steps):
        for c in range(col_blocks):
            out(i, c).wait()


def body(row_count, col_count, matrix):
    row_blocks, _, block, col_blocks, _, _ = matrix.shape
    grid = matrix.reshape(row_blocks, block, col_blocks, block)
    vec = (col_count, col_blocks, block)
    dma = pltpu.SemaphoreType.DMA
    span = max(row_blocks // 8, 1)
    batch = 4
    tile, left, right = pl.pallas_call(
        functools.partial(
            panel_kernel, row_count, col_count, row_blocks, col_blocks, block, batch
        ),
        out_shape=[
            pltpu.VMEM((col_blocks, row_blocks, block, block), jnp.float32),
            pltpu.VMEM((2 * K, row_blocks, block), jnp.float32),
            pltpu.VMEM((2 * K, col_blocks, block), jnp.float32),
        ],
        in_specs=[pl.BlockSpec(memory_space=pl.ANY)],
        out_specs=[pl.BlockSpec(memory_space=pltpu.VMEM)] * 3,
        scratch_shapes=[
            pltpu.VMEM((K,) + vec, jnp.float32),
            pltpu.VMEM((K,) + vec, jnp.float32),
            pltpu.VMEM((col_count, K + 1, col_blocks, block), jnp.float32),
            pltpu.VMEM((col_count // row_count, col_blocks, block, block), jnp.float32),
            pltpu.VMEM((K, col_blocks, block), jnp.float32),
            pltpu.VMEM((K,) + vec, jnp.float32),
            pltpu.VMEM((K,) + vec, jnp.float32),
            pltpu.VMEM(vec, jnp.float32),
            pltpu.VMEM(vec, jnp.float32),
            pltpu.VMEM(vec, jnp.float32),
            pltpu.VMEM((max(row_count, 8), block), jnp.float32),
            dma((col_blocks // batch,)),
            dma,
            dma((row_count, 2)),
            dma((2,)),
            dma((col_count, 2)),
            dma((col_count, 2)),
            dma((K, col_count)),
            dma((K, col_count)),
            dma((K, row_count)),
            dma((K, row_count)),
        ],
        compiler_params=pltpu.CompilerParams(
            collective_id=0, has_side_effects=True, vmem_limit_bytes=14 * 2**20
        ),
    )(grid)

    updated, images = pl.pallas_call(
        functools.partial(update_kernel, row_blocks, col_blocks, block, span),
        out_shape=[
            jax.ShapeDtypeStruct(grid.shape, jnp.float32),
            jax.ShapeDtypeStruct((K, row_blocks, block), jnp.float32),
        ],
        in_specs=[pl.BlockSpec(memory_space=pltpu.VMEM)] * 3,
        out_specs=[
            pl.BlockSpec(memory_space=pl.ANY),
            pl.BlockSpec(memory_space=pltpu.VMEM),
        ],
        scratch_shapes=[
            pltpu.VMEM((2, col_blocks, span, block, block), jnp.float32),
            pltpu.VMEM((6 * K, col_blocks * block), jnp.bfloat16),
            dma((2, col_blocks)),
        ],
        compiler_params=pltpu.CompilerParams(vmem_limit_bytes=14 * 2**20),
    )(tile, left, right)
    return (updated.reshape(matrix.shape), images.reshape(K, row_blocks, 1, block))


def solution(mesh):
    placed = (P(None, "row", None, None, "col", None),)
    return jax.shard_map(
        functools.partial(body, mesh.shape["row"], mesh.shape["col"]),
        mesh=mesh,
        in_specs=placed,
        out_specs=(P(None, "row", None, None, "col", None), P(None, None, "row", None)),
        check_vma=False,
    )
```

```python
import functools

import jax
import jax.numpy as jnp
from jax import lax
from jax.experimental import pallas as pl
from jax.experimental.pallas import tpu as pltpu
from jax.sharding import PartitionSpec as P

K = 8
epsilon = 1e-06
MESH = pl.DeviceIdType.MESH
WIDE = 16384.0


def total(values):
    rows = jnp.sum(values, axis=0)
    lanes = jnp.sum(rows, axis=0, keepdims=True)
    return jnp.sum(lanes, axis=1, keepdims=True)


def spread(value):
    return value.reshape(1, 1, 1)


def peak(values):
    rows = jnp.max(jnp.abs(values), axis=0)
    lanes = jnp.max(rows, axis=0, keepdims=True)
    return jnp.max(lanes, axis=1, keepdims=True)


def panel_kernel(
    row_count,
    col_count,
    row_blocks,
    col_blocks,
    block,
    batch,
    a_hbm,
    tile,
    left_ref,
    right_ref,
    v_ref,
    w_ref,
    pan,
    wide_ref,
    part,
    got,
    full,
    carry_ref,
    fix_ref,
    base_ref,
    rate_ref,
    head_ref,
    load_sem,
    own_sem,
    head_send,
    head_recv,
    down_send,
    down_recv,
    pan_send,
    pan_recv,
    part_send,
    part_recv,
    full_send,
    full_recv,
):
    p = lax.axis_index("row")
    q = lax.axis_index("col")
    ratio = col_count // row_count
    owner = lax.rem(q, row_count)
    rank = q // row_count
    mine = owner * ratio + rank
    local = owner == p
    span = batch * ratio
    groups = col_blocks // batch

    def load(i, c):
        blocks = pl.ds(i * span, span)
        return pltpu.make_async_copy(
            a_hbm.at[blocks, :, c], tile.at[c, blocks], load_sem.at[i]
        )

    own = pltpu.make_async_copy(a_hbm.at[0, pl.ds(0, K + 1)], pan.at[mine], own_sem)

    @pl.when(p == 0)
    def _():
        own.start()

    barrier = pltpu.get_barrier_semaphore()

    def greet(row, col):
        pl.semaphore_signal(barrier, inc=1, device_id=(row, col), device_id_type=MESH)

    for d in range(1, row_count):
        greet(lax.rem(p + d, row_count), q)
    for d in range(1, col_count):
        greet(p, lax.rem(q + d, col_count))
    for d in range(1, col_count):
        greet(owner, lax.rem(q + d, col_count))
    for r in range(row_count):
        for k in range(ratio):
            source = p + k * row_count

            @pl.when(jnp.logical_or(p != r, q != source))
            def _():
                greet(r, source)

    @pl.when(jnp.logical_not(local))
    def _():
        greet(owner, q)

    def start_load(i, carry):
        for c in range(col_blocks):
            load(i, c).start()
        return carry

    lax.fori_loop(0, groups, start_load, 0)
    v_ref[...] = jnp.zeros_like(v_ref)
    w_ref[...] = jnp.zeros_like(w_ref)
    carry_ref[...] = jnp.zeros_like(carry_ref)
    rate_ref[...] = jnp.ones_like(rate_ref)
    own_part = jnp.where(local, 1, 0)
    pl.semaphore_wait(barrier, row_count + col_count - 2 + 2 * (col_count - own_part))

    pieces = (pl.ds(0, 1), pl.ds(1, 1), pl.ds(2, K - 1))

    def head(d):
        return pltpu.make_async_remote_copy(
            src_ref=pan.at[mine, 0],
            dst_ref=head_ref.at[rank],
            send_sem=head_send.at[d],
            recv_sem=head_recv.at[rank],
            device_id=(owner, lax.rem(q + d, col_count)),
            device_id_type=MESH,
        )

    def head_wait(k):
        return pltpu.make_async_remote_copy(
            src_ref=pan.at[mine, 0],
            dst_ref=head_ref.at[k],
            send_sem=head_send.at[0],
            recv_sem=head_recv.at[k],
            device_id=(0, p + k * row_count),
            device_id_type=MESH,
        )

    def down(d, i):
        return pltpu.make_async_remote_copy(
            src_ref=pan.at[mine, pieces[i]],
            dst_ref=pan.at[mine, pieces[i]],
            send_sem=down_send.at[d, i],
            recv_sem=down_recv.at[i],
            device_id=(d, q),
            device_id_type=MESH,
        )

    def across(d, i, slot):
        return pltpu.make_async_remote_copy(
            src_ref=pan.at[slot, i],
            dst_ref=pan.at[slot, i],
            send_sem=pan_send.at[d, i],
            recv_sem=pan_recv.at[slot, i],
            device_id=(p, lax.rem(q + d, col_count)),
            device_id_type=MESH,
        )

    def across_recv(i):
        for d in range(1, col_count):
            other = lax.rem(q + d, col_count)
            across(d, i, lax.rem(other, row_count) * ratio + other // row_count).wait_recv()

    @pl.when(p == 0)
    def _():
        own.wait()
        for d in range(1, col_count):
            head(d).start()

    lone = jnp.logical_and(p == 0, local)

    @pl.when(jnp.logical_and(p == 0, jnp.logical_not(local)))
    def _():
        head(0).start()

    @pl.when(lone)
    def _():
        head_ref[rank] = pan[mine, 0]

    @pl.when(p == 0)
    def _():
        for i in range(3):
            for d in range(1, row_count):
                down(d, i).start()

    for i in range(2):

        @pl.when(p != 0)
        def _():
            down(0, i).wait_recv()

        for d in range(1, col_count):
            across(d, i, mine).start()

    shape = (col_count, col_blocks, block)
    slot_id = lax.broadcasted_iota(jnp.int32, shape, 0)
    block_id = (
        lax.broadcasted_iota(jnp.int32, shape, 1) * col_count
        + lax.rem(slot_id, ratio) * row_count
        + slot_id // ratio
    )
    ids = block_id * block + lax.broadcasted_iota(jnp.int32, shape, 2)
    lane = lax.broadcasted_iota(jnp.int32, (1, block), 1)
    def entry(row, i):
        return jnp.sum(jnp.where(lane == i, row, 0.0), axis=1, keepdims=True)

    def keep(ref, t, left_row, right_row):
        for k in range(ratio):
            left_ref[left_row, pl.ds(k, col_blocks, stride=ratio), :] = ref[t, p * ratio + k]
        right_ref[right_row] = ref[t, mine]

    def reflect(column, j):
        below = jnp.where(ids > j, column, 0.0)
        norm = jnp.sqrt(total(below * below))
        first = entry(column[0, 0:1, :], j + 1)
        denom = jnp.sqrt(2.0 * norm * (norm + first) + epsilon)
        u = (below + jnp.where(ids == j + 1, spread(norm), 0.0)) / spread(denom)
        v_ref[j] = u
        keep(v_ref, j, j, K + j)
        return norm, denom


    def send_part(j, d):
        return pltpu.make_async_remote_copy(
            src_ref=part.at[j],
            dst_ref=got.at[j, p * ratio + rank],
            send_sem=part_send.at[j, d],
            recv_sem=part_recv.at[j, p * ratio + rank],
            device_id=(owner, lax.rem(q + d, col_count)),
            device_id_type=MESH,
        )

    def recv_part(j, r, k):
        slot = r * ratio + k
        return pltpu.make_async_remote_copy(
            src_ref=part.at[j],
            dst_ref=got.at[j, slot],
            send_sem=part_send.at[j, 0],
            recv_sem=part_recv.at[j, slot],
            device_id=(r, p + k * row_count),
            device_id_type=MESH,
        )

    def full_copy(j, d, slot):
        return pltpu.make_async_remote_copy(
            src_ref=full.at[j, pl.ds(slot * ratio, ratio)],
            dst_ref=full.at[j, pl.ds(slot * ratio, ratio)],
            send_sem=full_send.at[j, d],
            recv_sem=full_recv.at[j, slot],
            device_id=(lax.rem(p + d, row_count), q),
            device_id_type=MESH,
        )

    def full_wait(j):
        for d in range(1, row_count):
            full_copy(j, d, lax.rem(p + d, row_count)).wait_recv()

    def image_of(i):
        u = v_ref[i]
        product = full[i] + carry_ref[...]
        image = product - fix_ref[...]
        gamma = total(u * image)
        update = 2.0 * image - spread(2.0 * gamma) * u
        w_ref[i] = update
        keep(w_ref, i, K + i, i)
        return u, product, gamma, update

    def widen(k, turned):
        for b in range(col_blocks):
            wide_ref[k, b] = jnp.broadcast_to(turned[:, b : b + 1], (block, block))

    def gather(b, k, acc):
        out = list(acc)
        a = b * ratio + k
        for r in range(0, block, 8):
            scale = wide_ref[k, b, r : r + 8, :]
            for c in range(col_blocks):
                out[c] = out[c] + tile[c, a, r : r + 8, :] * scale
        return tuple(out)

    blank = tuple(jnp.zeros((8, block), jnp.float32) for _ in range(col_blocks))

    def emit(j, acc):
        for c in range(col_blocks):
            part[j, c : c + 1, :] = jnp.sum(acc[c], axis=0, keepdims=True)
        for d in range(1, col_count):
            send_part(j, d).start()

        @pl.when(jnp.logical_not(local))
        def _():
            send_part(j, 0).start()

        @pl.when(local)
        def _():
            got[j, mine] = part[j]

    def positive(value):
        return jnp.where(value > 0.0, value, 1.0)

    def places(k):
        blocks = lax.broadcasted_iota(jnp.int32, shape[1:], 0) * col_count + k * row_count + p
        return blocks * block + lax.broadcasted_iota(jnp.int32, shape[1:], 1)

    firsts = []
    for k in range(ratio):

        @pl.when(jnp.logical_or(p != 0, q != p + k * row_count))
        def _():
            head_wait(k).wait_recv()

        firsts.append(jnp.where(places(k) > 0, head_ref[k], 0.0))
    first_top = functools.reduce(jnp.maximum, [peak(values[None]) for values in firsts])
    for k in range(ratio):
        widen(k, firsts[k].T * ((1.0 / WIDE) / positive(first_top)))

    def opening(g, acc):
        blocks = pl.ds(g * span, span)
        pltpu.make_async_copy(tile.at[:, blocks], tile.at[:, blocks], load_sem.at[g]).wait()
        for k in range(ratio):
            acc = lax.fori_loop(
                0, batch, lambda e, acc, k=k: gather(g * batch + e, k, acc), acc, unroll=2
            )
        return acc

    emit(0, lax.fori_loop(0, groups, opening, blank))

    def gap(k):
        ahead = lax.rem(p + k * row_count - q + col_count, col_count)
        return jnp.minimum(ahead, col_count - ahead)

    first_rank, nearest = 0, gap(0)
    for k in range(1, ratio):
        first_rank = jnp.where(gap(k) < nearest, k, first_rank)
        nearest = jnp.minimum(gap(k), nearest)

    def absorb(j, k):
        for r in range(row_count):

            @pl.when(jnp.logical_or(p != r, q != p + k * row_count))
            def _():
                recv_part(j, r, k).wait_recv()

        new = got[j, k] * rate_ref[0:1, :]
        for r in range(1, row_count):
            new = new + got[j, r * ratio + k] * rate_ref[r : r + 1, :]
        full[j, p * ratio + k] = new
        return new

    def share(j):
        for d in range(1, row_count):
            full_copy(j, d, p).start()

    def settle(inner, denom):
        for r in range(row_count):
            top = positive(peak(inner[r * ratio : (r + 1) * ratio]))
            rate_ref[r : r + 1, :] = jnp.broadcast_to(top * (WIDE / denom), (1, block))

    def step(j, beta):
        across_recv(j + 1)

        @pl.when(j == 0)
        def _():
            across_recv(0)
            norm, denom = reflect(pan[:, 0], 0)
            carry_ref[...] = spread(norm / denom) * pan[:, 1]
            settle(jnp.where(ids > 0, pan[:, 0], 0.0), denom)

        @pl.when(j > 0)
        def _():
            i = j - 1
            full_wait(i)
            trial = base_ref[...] - spread(beta) * full[i]
            inner = jnp.where(ids > j, trial, 0.0)
            u, product, gamma, update = image_of(i)
            sigma = beta * gamma - entry(update[0, 0:1, :], j)
            norm, denom = reflect(trial + spread(sigma) * u, j)
            carry_ref[...] = spread(sigma / denom) * (
                product - spread(0.5 * beta) * pan[:, j]
            ) + spread(norm / denom) * pan[:, j + 1]
            settle(inner, denom)

        u = v_ref[j]
        beta = 2.0 * entry(u[0, 0:1, :], j + 1)
        fix = jnp.zeros(shape, jnp.float32)
        column = pan[:, j + 1]
        for t in range(K):
            v_t, w_t = v_ref[t], w_ref[t]
            fix = fix + v_t * spread(total(w_t * u)) + w_t * spread(total(v_t * u))
            v_j = entry(v_ref[t, 0, 0:1, :], j + 1)
            w_j = entry(w_ref[t, 0, 0:1, :], j + 1)
            column = column - v_t * spread(w_j) - w_t * spread(v_j)
        fix_ref[...] = fix
        base_ref[...] = column + spread(beta) * (fix - carry_ref[...])

        @pl.when(j < K - 1)
        def _():
            acc, top = blank, None
            for h in range(ratio):
                k = lax.rem(first_rank + h, ratio)
                new = absorb(j, k)
                if h == ratio - 1:
                    share(j)

                    @pl.when(jnp.logical_and(p != 0, j == 0))
                    def _():
                        down(0, 2).wait_recv()

                    for d in range(1, col_count):
                        across(d, j + 2, mine).start()
                values = jnp.where(places(k) > j + 1, base_ref[p * ratio + k] - beta * new, 0.0)
                here = peak(values[None])
                if top is None:
                    top = here
                else:
                    old = positive(top)
                    top = jnp.maximum(top, here)
                    shrink = old / positive(top)
                    acc = tuple(value * shrink for value in acc)
                widen(k, values.T * ((1.0 / WIDE) / positive(top)))
                acc = lax.fori_loop(0, col_blocks, lambda b, acc, k=k: gather(b, k, acc), acc, unroll=2)
            emit(j + 1, acc)

        @pl.when(j == K - 1)
        def _():
            for k in range(ratio):
                absorb(j, k)
            share(j)

        return beta

    lax.fori_loop(0, K, step, jnp.zeros((1, 1), jnp.float32))
    full_wait(K - 1)
    image_of(K - 1)

    def drain(j, carry):
        for d in range(1, row_count):
            full_copy(j, d, p).wait_send()
        for d in range(1, col_count):
            send_part(j, d).wait_send()

        @pl.when(jnp.logical_not(local))
        def _():
            send_part(j, 0).wait_send()

        return carry

    lax.fori_loop(0, K, drain, 0)

    def drain_across(i, carry):
        for d in range(1, col_count):
            across(d, i, mine).wait_send()
        return carry

    lax.fori_loop(0, K + 1, drain_across, 0)

    @pl.when(p == 0)
    def _():
        for d in range(1, col_count):
            head(d).wait_send()
        for i in range(3):
            for d in range(1, row_count):
                down(d, i).wait_send()

    @pl.when(jnp.logical_and(p == 0, jnp.logical_not(local)))
    def _():
        head(0).wait_send()


def split(values):
    high = values.astype(jnp.bfloat16)
    low = (values - high.astype(jnp.float32)).astype(jnp.bfloat16)
    return high, low


def update_kernel(
    row_blocks, col_blocks, block, span, tile, left_ref, right_ref, out_hbm, image_ref, buf, thin, sem
):
    image_ref[...] = left_ref[K:]
    for c in range(col_blocks):
        high, low = split(right_ref[:, c, :])
        thin[:, c * block : (c + 1) * block] = jnp.concatenate([high, low, high], axis=0)

    def out(i, c):
        slot = lax.rem(i, 2)
        return pltpu.make_async_copy(
            buf.at[slot, c], out_hbm.at[pl.ds(i * span, span), :, c], sem.at[slot, c]
        )

    def chunk(i, carry):
        slot = lax.rem(i, 2)

        @pl.when(i >= 2)
        def _():
            for c in range(col_blocks):
                out(i - 2, c).wait()

        for s in range(span):
            high, low = split(left_ref[:, i * span + s, :])
            left = jnp.concatenate([high, high, low], axis=0)
            for c in range(0, col_blocks, 2):
                change = lax.dot_general(
                    left,
                    thin[:, c * block : (c + 2) * block],
                    (((0,), (0,)), ((), ())),
                    preferred_element_type=jnp.float32,
                )
                for e in range(2):
                    buf[slot, c + e, s] = (
                        tile[c + e, i * span + s] - change[:, e * block : (e + 1) * block]
                    )
        for c in range(col_blocks):
            out(i, c).start()
        return carry

    steps = row_blocks // span
    lax.fori_loop(0, steps, chunk, 0)
    for i in range(max(steps - 2, 0), steps):
        for c in range(col_blocks):
            out(i, c).wait()


def body(row_count, col_count, matrix):
    row_blocks, _, block, col_blocks, _, _ = matrix.shape
    grid = matrix.reshape(row_blocks, block, col_blocks, block)
    vec = (col_count, col_blocks, block)
    dma = pltpu.SemaphoreType.DMA
    span = max(row_blocks // 8, 1)
    batch = 4
    tile, left, right = pl.pallas_call(
        functools.partial(
            panel_kernel, row_count, col_count, row_blocks, col_blocks, block, batch
        ),
        out_shape=[
            pltpu.VMEM((col_blocks, row_blocks, block, block), jnp.float32),
            pltpu.VMEM((2 * K, row_blocks, block), jnp.float32),
            pltpu.VMEM((2 * K, col_blocks, block), jnp.float32),
        ],
        in_specs=[pl.BlockSpec(memory_space=pl.ANY)],
        out_specs=[pl.BlockSpec(memory_space=pltpu.VMEM)] * 3,
        scratch_shapes=[
            pltpu.VMEM((K,) + vec, jnp.float32),
            pltpu.VMEM((K,) + vec, jnp.float32),
            pltpu.VMEM((col_count, K + 1, col_blocks, block), jnp.float32),
            pltpu.VMEM((col_count // row_count, col_blocks, block, block), jnp.float32),
            pltpu.VMEM((K, col_blocks, block), jnp.float32),
            pltpu.VMEM((K,) + vec, jnp.float32),
            pltpu.VMEM((K,) + vec, jnp.float32),
            pltpu.VMEM(vec, jnp.float32),
            pltpu.VMEM(vec, jnp.float32),
            pltpu.VMEM(vec, jnp.float32),
            pltpu.VMEM((max(row_count, 8), block), jnp.float32),
            pltpu.VMEM((col_count // row_count, col_blocks, block), jnp.float32),
            dma((col_blocks // batch,)),
            dma,
            dma((col_count,)),
            dma((col_count // row_count,)),
            dma((row_count, 3)),
            dma((3,)),
            dma((col_count, K + 1)),
            dma((col_count, K + 1)),
            dma((K, col_count)),
            dma((K, col_count)),
            dma((K, row_count)),
            dma((K, row_count)),
        ],
        compiler_params=pltpu.CompilerParams(
            collective_id=0, has_side_effects=True, vmem_limit_bytes=14 * 2**20
        ),
    )(grid)

    updated, images = pl.pallas_call(
        functools.partial(update_kernel, row_blocks, col_blocks, block, span),
        out_shape=[
            jax.ShapeDtypeStruct(grid.shape, jnp.float32),
            jax.ShapeDtypeStruct((K, row_blocks, block), jnp.float32),
        ],
        in_specs=[pl.BlockSpec(memory_space=pltpu.VMEM)] * 3,
        out_specs=[
            pl.BlockSpec(memory_space=pl.ANY),
            pl.BlockSpec(memory_space=pltpu.VMEM),
        ],
        scratch_shapes=[
            pltpu.VMEM((2, col_blocks, span, block, block), jnp.float32),
            pltpu.VMEM((6 * K, col_blocks * block), jnp.bfloat16),
            dma((2, col_blocks)),
        ],
        compiler_params=pltpu.CompilerParams(vmem_limit_bytes=14 * 2**20),
    )(tile, left, right)
    return (updated.reshape(matrix.shape), images.reshape(K, row_blocks, 1, block))


def solution(mesh):
    placed = (P(None, "row", None, None, "col", None),)
    return jax.shard_map(
        functools.partial(body, mesh.shape["row"], mesh.shape["col"]),
        mesh=mesh,
        in_specs=placed,
        out_specs=(P(None, "row", None, None, "col", None), P(None, None, "row", None)),
        check_vma=False,
    )
```
